256 devices in a mesh: tm: 8 (over x, core), row: 32 (over z, y).
Axes of the slice: x: 4, y: 4, z: 8, core: 2. Of those that a mesh axis runs over, the one named last changes fastest.
Arguments:
- image: float32 [8, 1, 2048, 2048], P('tm', None, 'row'), may hold values from -6 to 6
- relaxed: float32 [8, 1, 2048, 2048], P('tm', None, 'row'), may hold values from -6 to 6
- dual: float32 [8, 1, 2048, 2048], P('tm', None, 'row'), may hold values from -2 to 2
- sinogram: float32 [8, 12, 1, 2048], P('tm'), may hold values from -48 to 48
- angle_index: int32 [8, 12], P('tm'), may hold values from 0 to 31, as said below
- bin_offset: int32 [128, 32], P('row'), may hold values from 0 to 2047
- row_weight: float32 [32, 16], replicated, may hold values from 0.5 to 1.5
- response: bfloat16 [32, 128, 128], replicated, may hold values from -0.5 to 0.5
- row_gain: float32 [2048], P('row'), may hold values from 0.6 to 11.2
Outputs:
- image_new: float32 [8, 1, 2048, 2048], P('tm', None, 'row')
- dual_new: float32 [8, 1, 2048, 2048], P('tm', None, 'row')
The draws below stay inside these ranges and needn't reach their ends.
Inputs may be any that keep to these rules, and one draw needn't show every extreme that they name: `angle_index`: the 12 views of one phase name distinct entries of the angle table.
All inputs are finite; a program needn't handle non-finite values.
Results may differ from the reference program's by a relative error of at most 0.0003.
Values sent between devices are 32-bit elements; how exact they have to be, the bound alone decides.
A program may use at most 64 MiB of HBM per device.

```python
import jax
import jax.numpy as jnp
from jax import lax

COLS = 2048
BLK = 128
SLICES = 1
TR = 16
VIEWS = 12
NANG = 32
CG_ITERS = 3
PHASES = 8
ROWS = 2048
TILES = 128


def draw_angle_index(key, part):
    keys = jax.random.split(jax.random.fold_in(key, 11), PHASES)

    def order(single):
        return jax.random.permutation(single, NANG)
    orders = jax.vmap(order)(keys)
    return orders[:, :VIEWS].astype(jnp.int32)


def draw_row_gain(key, part):
    position = jnp.arange(ROWS, dtype=jnp.float32) / float(max(ROWS - 1, 1))
    rough = jax.random.uniform(jax.random.fold_in(key, 23), (ROWS,), jnp.float32, 0.6, 1.4)
    rising = 4.0
    return (jnp.exp(jnp.log(rising) * position) * rough).astype(jnp.float32)


def plant(values, key, low, largest):
    longest = values.shape.index(max(values.shape))
    spots = []
    for shift in (0, 1):
        where = [jax.random.randint(jax.random.fold_in(key, axis), (), 0, length) for axis, length in enumerate(values.shape)]
        where[longest] = (where[longest] + shift) % values.shape[longest]
        spots.append(tuple(where))
    return values.at[spots[0]].set(low).at[spots[1]].set(largest)


def block_scale(stream_key, shape, cuts, low, high):
    level, own = 1.0, jax.random.fold_in(stream_key, 6)
    for dim, shards_of in cuts:
        heights = jnp.exp(jax.random.uniform(jax.random.fold_in(own, dim), (shards_of,), jnp.float32, low / len(cuts), high / len(cuts)))
        level = level * jnp.repeat(heights, shape[dim] // shards_of).reshape([-1 if axis == dim else 1 for axis in range(len(shape))])
    return level


def noise(stream_key, shape, deviation, bound, cuts=(), held_as=jnp.bfloat16):
    drawn = jax.random.normal(stream_key, shape, jnp.float32) * deviation
    if len(cuts) > 0:
        drawn = block_scale(stream_key, shape, cuts, -0.22, 0.18) * drawn
    return jnp.clip(drawn, min=-bound, max=bound).astype(held_as)


def setup_inputs(seed: int = 0) -> dict:
    arg_keys = jax.random.split(jax.random.key(seed), 10)
    return {
        "image": noise(arg_keys[0], (PHASES, SLICES, ROWS, COLS), 1.0, 6.0, ((0, 8), (2, 32)), jnp.float32),
        "relaxed": noise(arg_keys[1], (PHASES, SLICES, ROWS, COLS), 1.0, 6.0, ((0, 8), (2, 32)), jnp.float32),
        "dual": jnp.clip(jax.random.uniform(arg_keys[2], (PHASES, SLICES, ROWS, COLS), jnp.float32, -2.0, 2.0) * block_scale(arg_keys[2], (PHASES, SLICES, ROWS, COLS), ((0, 8), (2, 32)), -0.4, 0.0), -2.0, 2.0),
        "sinogram": noise(arg_keys[3], (PHASES, VIEWS, SLICES, COLS), 8.0, 48.0, ((0, 8),), jnp.float32),
        "angle_index": draw_angle_index(jax.random.fold_in(arg_keys[9], 71), 0),
        "bin_offset": plant(jax.random.randint(arg_keys[5], (TILES, NANG), 0, COLS), jax.random.fold_in(arg_keys[5], 1), 0, COLS - 1).astype(jnp.int32),
        "row_weight": jnp.clip(jax.random.uniform(arg_keys[6], (NANG, TR), jnp.float32, 0.5, 1.5), 0.5, 1.5),
        "response": noise(arg_keys[7], (NANG, BLK, BLK), BLK ** -0.5, 0.5),
        "row_gain": draw_row_gain(jax.random.fold_in(arg_keys[9], 71), 0),
    }


HIGH = lax.Precision.HIGHEST
TAU_STEP = 0.1
SIGMA_STEP = 2.0
LAMBDA_BOUND = 2.0


def view_tables(angles, row_weight, response, bin_offset):
    selector = angles[:, None] == jnp.arange(row_weight.shape[0], dtype=jnp.int32)[None, :]
    chosen = selector.astype(jnp.float32)
    weights = jnp.dot(chosen, row_weight, precision=HIGH)
    blocks = jnp.einsum('va,aio->vio', chosen, response.astype(jnp.float32), precision=HIGH)
    shifts = jnp.sum(jnp.where(selector[None, :, :], bin_offset[:, None, :], 0), axis=2).astype(jnp.int32)
    return weights, blocks, shifts


def shift_columns(rows, start):
    width = rows.shape[-1]
    doubled = jnp.concatenate([rows, rows], axis=-1)
    return lax.dynamic_slice_in_dim(doubled, start.astype(jnp.int32), width, axis=rows.ndim - 1)


def spread_view(rows, starts):
    width = rows.shape[-1]
    doubled = jnp.concatenate([rows, rows], axis=-1)

    def pick(start):
        return lax.dynamic_slice_in_dim(doubled, start.astype(jnp.int32), width, axis=rows.ndim - 1)

    return jax.vmap(pick)(starts)


def project(volume, weights, blocks, shifts):
    num_slices, num_rows, num_cols = volume.shape
    num_views, tile_rows = weights.shape
    block_width = blocks.shape[1]
    tile_count = num_rows // tile_rows
    tiled = volume.reshape(num_slices, tile_count, tile_rows, num_cols)
    summed = jnp.einsum('vj,skjc->vksc', weights, tiled, precision=HIGH)
    blocked = summed.reshape(num_views, tile_count, num_slices, num_cols // block_width, block_width)
    mapped = jnp.einsum('vksni,vio->vksno', blocked, blocks, precision=HIGH)
    mapped = mapped.reshape(num_views, tile_count, num_slices, num_cols)
    starts = ((num_cols - jnp.transpose(shifts)) % num_cols).astype(jnp.int32)
    rolled = jax.vmap(jax.vmap(shift_columns))(mapped, starts)
    return jnp.sum(rolled, axis=1)


def backproject(projected, weights, blocks, shifts):
    num_views, num_slices, num_cols = projected.shape
    tile_rows = weights.shape[1]
    block_width = blocks.shape[1]
    tile_count = shifts.shape[0]
    starts = (jnp.transpose(shifts) % num_cols).astype(jnp.int32)
    picked = jax.vmap(spread_view)(projected, starts)
    blocked = picked.reshape(num_views, tile_count, num_slices, num_cols // block_width, block_width)
    mapped = jnp.einsum('vksno,vio->vksni', blocked, blocks, precision=HIGH)
    mapped = mapped.reshape(num_views, tile_count, num_slices, num_cols)
    tiled = jnp.einsum('vj,vksc->skjc', weights, mapped, precision=HIGH)
    return tiled.reshape(num_slices, tile_count * tile_rows, num_cols)


def reference(image, relaxed, dual, sinogram, angle_index, bin_offset, row_weight, response, row_gain):
    dual_new = jnp.clip(dual + SIGMA_STEP * (jnp.roll(relaxed, -1, axis=0) - relaxed), -LAMBDA_BOUND, LAMBDA_BOUND)
    primal = image - TAU_STEP * (jnp.roll(dual_new, 1, axis=0) - dual_new)
    gain = row_gain[None, :, None]

    def solve_phase(inputs):
        start, measured, angles = inputs
        weights, blocks, shifts = view_tables(angles, row_weight, response, bin_offset)

        def forward(volume):
            return project(volume * gain, weights, blocks, shifts)

        def adjoint(projected):
            return backproject(projected, weights, blocks, shifts) * gain

        def normal(direction):
            return adjoint(forward(direction)) + direction / TAU_STEP

        solution = start
        resid = adjoint(measured - forward(start))
        direction = resid
        norm_now = jnp.sum(resid * resid)
        for step in range(CG_ITERS):
            image_w = normal(direction)
            alpha = norm_now / jnp.sum(direction * image_w)
            solution = solution + alpha * direction
            resid = resid - alpha * image_w
            norm_next = jnp.sum(resid * resid)
            direction = resid + (norm_next / norm_now) * direction
            norm_now = norm_next
        return solution

    image_new = lax.map(solve_phase, (primal, sinogram, angle_index))
    return image_new, dual_new
```

```python
import jax
import jax.numpy as jnp
from jax import lax
from jax.experimental import pallas as pl
from jax.experimental.pallas import tpu as pltpu
from jax.sharding import PartitionSpec as P

MESH = pl.DeviceIdType.MESH
F32 = jnp.float32
BF16 = jnp.bfloat16

CG_ITERS = 3
TAU_STEP = 0.1
SIGMA_STEP = 2.0
LAMBDA_BOUND = 2.0

COLS = 2048
BLK = 128
NB = COLS // BLK
TR = 16
VIEWS = 12
VPAD = 16
HALVES = 2 * VIEWS
NZ, NY = 8, 4
NR = NZ * NY
GROUP = 2 * NY
GROUP_ROWS = NR // GROUP
CHUNKS = HALVES // GROUP
PAIRS = 80
ROUNDS = NZ // 2 + NY // 2 - 1
VMEM_LIMIT = 60 * 1024 * 1024

OTHERS = sorted(
    ((dz, dy) for dz in range(NZ) for dy in range(NY) if dz or dy),
    key=lambda d: -(min(d[0], NZ - d[0]) + min(d[1], NY - d[1])),
)
MEMBERS = sorted(
    ((dz, dy) for dz in range(2) for dy in range(NY) if dz or dy),
    key=lambda d: -(d[0] + min(d[1], NY - d[1])),
)


def split(x):
    hi = x.astype(BF16)
    lo = (x - hi.astype(F32)).astype(BF16)
    return hi, lo


def small_dot(a, b):
    ah, al = split(a)
    bh, bl = split(b)
    return jnp.dot(
        jnp.concatenate([ah, ah, al], axis=1),
        jnp.concatenate([bh, bl, bh], axis=0),
        preferred_element_type=F32,
    )


def solve_kernel(
    angles, offsets,
    image, relaxed, dual, sinogram, row_weight, response, gain, offsets_v,
    x0_out, step_out, next_out,
    img, rel, dua, rel_next, s_own, s_prev, resp, sino,
    table, wts, pairs, dg, rf, rt, dbl, lhs, mapped, mix, ys,
    part, total, got, got_group, rho, pi, gpi, xi,
    off_own, off_all, gain_own, gain_all, off_group, far_in, turn,
    load_sem, misc_sem, round_sem, rel_send, rel_recv, s_send, s_recv,
    tab_send, tab_recv, rs_send, rs_recv, ag_send, ag_recv, grs_send, grs_recv, gag_send, gag_recv, *tmp,
):
    nt = lax.axis_size("tm")
    t, me = lax.axis_index("tm"), lax.axis_index("row")
    after, before = lax.rem(t + 1, nt), lax.rem(t + nt - 1, nt)
    z, y = me // NY, lax.rem(me, NY)
    low = lax.rem(z, 2)
    place_in_group = low * NY + y
    tiles = img.shape[0]
    group_tiles = tiles * NR // GROUP
    lane = lax.broadcasted_iota(jnp.int32, (NB, BLK), 1)

    def there(dz, dy):
        return lax.rem(z + dz, NZ) * NY + lax.rem(y + dy, NY)

    def source(dz, dy):
        return there(NZ - dz, NY - dy)

    def load(i, k):
        src, dst = ((relaxed, rel), (dual, dua), (image, img))[i]
        return pltpu.make_async_copy(src.at[pl.ds(k * TR, TR), :], dst.at[k], load_sem.at[i, k])

    for k in range(tiles):
        load(0, k).start()
        load(1, k).start()

    near = [there(1, 0), there(NZ - 1, 0), there(0, 1), there(0, NY - 1)]
    barrier = pltpu.get_barrier_semaphore()
    for other in (after, before):
        pl.semaphore_signal(barrier, inc=1, device_id=(other, me), device_id_type=MESH)
    for other in near:
        pl.semaphore_signal(barrier, inc=1, device_id=(t, other), device_id_type=MESH)
    fetch_resp = pltpu.make_async_copy(response, resp, misc_sem.at[0])
    fetch_resp.start()
    for k in range(tiles):
        load(2, k).start()
    fetch_sino = pltpu.make_async_copy(sinogram, sino, misc_sem.at[1])
    fetch_sino.start()
    pl.semaphore_wait(barrier, len(near) + 2)

    rel_copies = [
        pltpu.make_async_remote_copy(
            rel.at[k], rel_next.at[k], rel_send.at[k], rel_recv.at[k],
            device_id=(before, me), device_id_type=MESH,
        )
        for k in range(tiles)
    ]
    s_copies = [
        pltpu.make_async_remote_copy(
            s_own.at[k], s_prev.at[k], s_send.at[k], s_recv.at[k],
            device_id=(after, me), device_id_type=MESH,
        )
        for k in range(tiles)
    ]
    for k in range(tiles):
        load(0, k).wait()
        rel_copies[k].start()
        load(1, k).wait()
        s_own[k] = dua[k] - SIGMA_STEP * rel[k]
        if k > 0:
            s_copies[k - 1].start()
    off_own[0:tiles, 0 : offsets_v.shape[1]] = offsets_v[...]
    gain_own[0:1, 0 : gain.shape[1]] = gain[...]
    s_copies[tiles - 1].start()

    for i in range(ROUNDS):
        for other in near:
            pl.semaphore_signal(round_sem.at[i], inc=1, device_id=(t, other), device_id_type=MESH)
        if i == 0:
            fetch_resp.wait()
            wts[...] = jnp.zeros_like(wts)
            table[...] = jnp.transpose(row_weight[...])
            for v in range(VIEWS):
                a = angles[0, v]
                wts[v : v + 1, :] = table[pl.ds(a, 1), :]
                r = resp[a]
                rf[v, 0:BLK, :] = r
                rf[v, BLK : 2 * BLK, :] = r
                flipped = jnp.transpose(r.astype(F32)).astype(BF16)
                rt[v, 0:BLK, :] = flipped
                rt[v, BLK : 2 * BLK, :] = flipped
            for k in range(tiles):
                dg[k] = wts[...] * gain[:, k * TR : (k + 1) * TR]
            ys[...] = jnp.zeros_like(ys)
            pairs[...] = jnp.zeros_like(pairs)
            row = 0
            for v in range(VIEWS):
                pairs[row : row + VIEWS - v, :] = wts[v : v + 1, :] * wts[v:VIEWS, :]
                row += VIEWS - v
        pl.semaphore_wait(round_sem.at[i], len(near))

    share = GROUP_ROWS
    taker, slot_there = me // share, lax.rem(me, share)

    def tables(g):
        other = g * GROUP + taker
        return [
            pltpu.make_async_remote_copy(
                own, every.at[slot_there], tab_send.at[i, g], tab_recv.at[i, slot_there],
                device_id=(t, other), device_id_type=MESH,
            )
            for i, (own, every) in enumerate(((off_own, off_all), (gain_own, gain_all)))
        ]

    for g in range(NR // GROUP):
        @pl.when(g * GROUP + taker != me)
        def _(g=g):
            for c in tables(g):
                c.start()

    def arrived(i, j):
        own, every = ((off_own, off_all), (gain_own, gain_all))[i]
        return pltpu.make_async_remote_copy(
            own, every.at[j], tab_send.at[i, 0], tab_recv.at[i, j],
            device_id=(t, me), device_id_type=MESH,
        )

    def group_tables():
        for j in range(share):
            @pl.when(place_in_group * share + j != me)
            def _(j=j):
                arrived(0, j).wait_recv()
                arrived(1, j).wait_recv()

            @pl.when(place_in_group * share + j == me)
            def _(j=j):
                off_all[j] = off_own[...]
                gain_all[j] = gain_own[...]
        to_smem = pltpu.make_async_copy(off_all, off_group, misc_sem.at[2])
        to_smem.start()
        ph, plo = split(pairs[...])
        stacked = jnp.concatenate([ph, ph, plo], axis=1)
        for j in range(share):
            column = jnp.transpose(gain_all[j])[0 : tiles * TR, 0:1]
            squares = jnp.broadcast_to(column * column, (tiles * TR, BLK))
            for k in range(tiles):
                gh, gl = split(squares[k * TR : (k + 1) * TR])
                mix[j * tiles + k] = jnp.dot(
                    stacked, jnp.concatenate([gh, gl, gh], axis=0), preferred_element_type=F32
                )
        for g in range(NR // GROUP):
            @pl.when(g * GROUP + taker != me)
            def _(g=g):
                for c in tables(g):
                    c.wait_send()
        to_smem.wait()
        for k in range(group_tiles):
            for v in range(VIEWS):
                off = off_group[k // tiles, k % tiles, angles[0, v]]
                far_in[k * VIEWS + v] = lax.shift_right_logical(off, 7)
                turn[k * VIEWS + v] = off & (BLK - 1)

    def own_shift(k, v):
        off = offsets[k, angles[0, v]]
        return lax.shift_right_logical(off, 7), off & (BLK - 1)

    def group_shift(k, v):
        return far_in[k * VIEWS + v], turn[k * VIEWS + v]

    def roll_out(count, shift):
        for v in range(VIEWS):
            mapped[v, 0 : count * NB, :] = jnp.dot(
                lhs[v, 0 : count * NB, :], rf[v], preferred_element_type=F32
            )
        for v in range(VIEWS):
            twice = tmp[v]
            for k in range(count):
                turned = pltpu.roll(mapped[v, k * NB : (k + 1) * NB, :], shift(k, v)[1], 1)
                twice[k, 0:NB, :] = turned
                twice[k, NB : 2 * NB, :] = turned
            acc = None
            for k in range(count):
                q, r = shift(k, v)
                near_rows = twice[k, pl.ds(NB - q, NB), :]
                far_rows = twice[k, pl.ds(NB - 1 - q, NB), :]
                one = jnp.where(lane >= r, near_rows, far_rows)
                acc = one if acc is None else acc + one
            part[2 * v] = acc[0:8]
            part[2 * v + 1] = acc[8:16]

    def roll_back(w, count, shift):
        dbl[:, 0:NB, :] = w
        dbl[:, NB : 2 * NB, :] = w
        for v in range(VIEWS):
            for k in range(count):
                q, r = shift(k, v)
                near_rows = dbl[v, pl.ds(q, NB), :]
                far_rows = dbl[v, pl.ds(q + 1, NB), :]
                e = pltpu.roll(jnp.where(lane >= r, near_rows, far_rows), (BLK - r) & (BLK - 1), 1)
                hi, lo = split(e)
                lhs[v, k * NB : (k + 1) * NB, 0:BLK] = hi
                lhs[v, k * NB : (k + 1) * NB, BLK : 2 * BLK] = lo

    def scatter(i):
        other = there(*OTHERS[i])
        return pltpu.make_async_remote_copy(
            part.at[other], got.at[i], rs_send, rs_recv, device_id=(t, other), device_id_type=MESH
        )

    def gather(i):
        return pltpu.make_async_remote_copy(
            total.at[me], total.at[me], ag_send, ag_recv,
            device_id=(t, there(*OTHERS[i])), device_id_type=MESH,
        )

    def wait_for(chunks, sem):
        pltpu.make_async_copy(got.at[pl.ds(0, chunks)], got.at[pl.ds(0, chunks)], sem).wait()

    def sum_rows(meanwhile):
        for i in range(len(OTHERS)):
            @pl.when(there(*OTHERS[i]) < HALVES)
            def _(i=i):
                scatter(i).start()

        meanwhile()

        @pl.when(me < HALVES)
        def _():
            wait_for(NR - 1, rs_recv)
            acc = part[me]
            for i in range(len(OTHERS)):
                acc = acc + got[i]
            total[me] = acc
            for i in range(len(OTHERS)):
                gather(i).start()
            wait_for(HALVES - 1, rs_send)
            wait_for(HALVES - 1, ag_recv)
            wait_for(NR - 1, ag_send)

        @pl.when(me >= HALVES)
        def _():
            wait_for(HALVES, rs_send)
            wait_for(HALVES, ag_recv)

    def place(dz, dy):
        return lax.rem(low + dz, 2) * NY + lax.rem(y + dy, NY)

    def member(dz, dy):
        return (z - low) * NY + place(dz, dy)

    def group_scatter(dz, dy):
        i = dz * NY + dy
        return pltpu.make_async_remote_copy(
            part.at[pl.ds(place(dz, dy) * CHUNKS, CHUNKS)], got_group.at[i], grs_send.at[i], grs_recv.at[i],
            device_id=(t, member(dz, dy)), device_id_type=MESH,
        )

    def group_gather(dz, dy, owner):
        i = dz * NY + dy
        chunk = pl.ds(owner * CHUNKS, CHUNKS)
        return pltpu.make_async_remote_copy(
            total.at[chunk], total.at[chunk], gag_send.at[i], gag_recv.at[i],
            device_id=(t, member(dz, dy)), device_id_type=MESH,
        )

    def sum_group():
        for d in MEMBERS:
            group_scatter(*d).start()
        mine = pl.ds(place_in_group * CHUNKS, CHUNKS)
        acc = part[mine]
        for d in reversed(MEMBERS):
            group_scatter(*d).wait_recv()
            acc = acc + got_group[d[0] * NY + d[1]]
        total[mine] = acc
        for d in MEMBERS:
            group_gather(*d, place_in_group).start()
        for d in MEMBERS:
            group_scatter(*d).wait_send()
        for d in reversed(MEMBERS):
            group_gather(*d, place(2 - d[0], NY - d[1])).wait_recv()
        for d in MEMBERS:
            group_gather(*d, place_in_group).wait_send()

    def summed():
        return total[...].reshape(VIEWS, NB, BLK)

    for k in range(tiles):
        rows = pl.ds(k * TR, TR)
        s_copies[k].wait_recv()
        rel_copies[k].wait_recv()
        load(2, k).wait()
        behind = jnp.clip(s_prev[k] + SIGMA_STEP * rel[k], -LAMBDA_BOUND, LAMBDA_BOUND)
        ahead = jnp.clip(dua[k] + SIGMA_STEP * (rel_next[k] - rel[k]), -LAMBDA_BOUND, LAMBDA_BOUND)
        x0_out[rows, :] = img[k] - TAU_STEP * (behind - ahead)
        next_out[rows, :] = rel_next[k]
        zk = small_dot(dg[k], x0_out[rows, :])
        for n in range(NB):
            ys[pl.ds((k * NB + n) * VPAD, VPAD), :] = zk[:, n * BLK : (n + 1) * BLK]
    for v in range(VIEWS):
        hi, lo = split(ys[pl.ds(v, tiles * NB, stride=VPAD), :])
        lhs[v, 0 : tiles * NB, 0:BLK] = hi
        lhs[v, 0 : tiles * NB, BLK : 2 * BLK] = lo
    roll_out(tiles, own_shift)

    sum_rows(group_tables)
    fetch_sino.wait()
    rho[...] = sino[...] - summed()
    pi[...] = jnp.zeros_like(pi)
    gpi[...] = jnp.zeros_like(gpi)
    xi[...] = jnp.zeros_like(xi)

    def inner(a, b):
        return jnp.sum(jnp.sum(a * b, axis=0), keepdims=True)

    def mix_tile(k, _):
        rows = pl.ds(pl.multiple_of(k * NB, NB), NB)
        parts = [mapped[v, rows, :] for v in range(VIEWS)]
        sums = [None] * VIEWS
        row = 0
        for v in range(VIEWS):
            for w in range(v, VIEWS):
                c = mix[k, row : row + 1, :]
                row += 1
                for a, b in ((v, w), (w, v))[: 1 + (v != w)]:
                    term = c * parts[b]
                    sums[a] = term if sums[a] is None else sums[a] + term
        for v in range(VIEWS):
            hi, lo = split(sums[v])
            lhs[v, rows, 0:BLK] = hi
            lhs[v, rows, BLK : 2 * BLK] = lo
        return 0

    def step(it, norm_now):
        roll_back(rho[...], group_tiles, group_shift)
        for v in range(VIEWS):
            mapped[v] = jnp.dot(lhs[v], rt[v], preferred_element_type=F32)
        lax.fori_loop(0, group_tiles, mix_tile, 0)
        roll_out(group_tiles, group_shift)
        sum_group()
        g = summed()
        norm_next = inner(rho[...], g)
        beta = jnp.where(it == 0, 0.0, norm_next / norm_now)
        pi[...] = rho[...] + beta[None] * pi[...]
        gpi[...] = g + beta[None] * gpi[...]
        product = inner(gpi[...], gpi[...]) + inner(pi[...], gpi[...]) / TAU_STEP
        alpha = (norm_next / product)[None]
        xi[...] = xi[...] + alpha * pi[...]
        rho[...] = rho[...] - alpha * (gpi[...] + pi[...] / TAU_STEP)
        return norm_next

    lax.fori_loop(0, CG_ITERS, step, jnp.ones((1, 1), F32))

    roll_back(xi[...], tiles, own_shift)
    for v in range(VIEWS):
        ys[pl.ds(v, tiles * NB, stride=VPAD), :] = jnp.dot(
            lhs[v, 0 : tiles * NB, :], rt[v], preferred_element_type=F32
        )
    for k in range(tiles):
        yk = jnp.concatenate([ys[pl.ds((k * NB + n) * VPAD, VPAD), :] for n in range(NB)], axis=1)
        step_out[pl.ds(k * TR, TR), :] = small_dot(jnp.transpose(dg[k]), yk)
    for c in rel_copies + s_copies:
        c.wait_send()


def local(image, relaxed, dual, sinogram, angle_index, bin_offset, row_weight, response, row_gain):
    rows = image.shape[2]
    tiles = rows // TR
    group_tiles = tiles * NR // GROUP
    block = (tiles, TR, COLS)
    sino = (VIEWS, NB, BLK)
    any_ = pl.BlockSpec(memory_space=pl.ANY)
    vmem = pl.BlockSpec(memory_space=pltpu.VMEM)
    smem = pl.BlockSpec(memory_space=pltpu.SMEM)
    dma = pltpu.SemaphoreType.DMA
    x0, step, ahead = pl.pallas_call(
        solve_kernel,
        name="solve",
        out_shape=(pltpu.VMEM((rows, COLS), F32),) * 3,
        in_specs=[smem, smem, any_, any_, any_, any_, vmem, any_, vmem, vmem],
        out_specs=(vmem,) * 3,
        scratch_shapes=[pltpu.VMEM(block, F32)] * 6
        + [
            pltpu.VMEM(response.shape, BF16),
            pltpu.VMEM(sino, F32),
            pltpu.VMEM(row_weight.shape, F32),
            pltpu.VMEM((VPAD, TR), F32),
            pltpu.VMEM((PAIRS, TR), F32),
            pltpu.VMEM((tiles, VPAD, TR), F32),
            pltpu.VMEM((VIEWS, 2 * BLK, BLK), BF16),
            pltpu.VMEM((VIEWS, 2 * BLK, BLK), BF16),
            pltpu.VMEM((VIEWS, 2 * NB, BLK), F32),
            pltpu.VMEM((VIEWS, group_tiles * NB, 2 * BLK), BF16),
            pltpu.VMEM((VIEWS, group_tiles * NB, BLK), F32),
            pltpu.VMEM((group_tiles, PAIRS, BLK), F32),
            pltpu.VMEM((tiles * NB * VPAD, BLK), F32),
            pltpu.VMEM((HALVES, 8, BLK), F32),
            pltpu.VMEM((HALVES, 8, BLK), F32),
            pltpu.VMEM((NR - 1, 8, BLK), F32),
            pltpu.VMEM((GROUP, CHUNKS, 8, BLK), F32),
        ]
        + [pltpu.VMEM(sino, F32)] * 4
        + [
            pltpu.VMEM((8, BLK), jnp.int32),
            pltpu.VMEM((GROUP_ROWS, 8, BLK), jnp.int32),
            pltpu.VMEM((8, BLK), F32),
            pltpu.VMEM((GROUP_ROWS, 8, BLK), F32),
            pltpu.SMEM((GROUP_ROWS, 8, BLK), jnp.int32),
            pltpu.SMEM((group_tiles * VIEWS,), jnp.int32),
            pltpu.SMEM((group_tiles * VIEWS,), jnp.int32),
        ]
        + [dma((3, tiles)), dma((3,)), pltpu.SemaphoreType.REGULAR((ROUNDS,))]
        + [dma((tiles,))] * 4
        + [dma((2, NR // GROUP)), dma((2, GROUP_ROWS))]
        + [dma(())] * 4
        + [dma((GROUP,))] * 4
        + [pltpu.VMEM((group_tiles, 2 * NB, BLK), F32)] * VIEWS,
        compiler_params=pltpu.CompilerParams(
            collective_id=0, has_side_effects=True, vmem_limit_bytes=VMEM_LIMIT
        ),
    )(
        angle_index,
        bin_offset,
        image.reshape(rows, COLS),
        relaxed.reshape(rows, COLS),
        dual.reshape(rows, COLS),
        sinogram.reshape(sino),
        jnp.transpose(row_weight),
        response,
        row_gain.reshape(1, rows),
        bin_offset,
    )
    image_new = (x0 + step).reshape(image.shape)
    ahead = ahead.reshape(image.shape)
    dual_new = jnp.clip(dual + SIGMA_STEP * (ahead - relaxed), -LAMBDA_BOUND, LAMBDA_BOUND)
    return image_new, dual_new


def solution(mesh):
    return jax.shard_map(
        local,
        mesh=mesh,
        in_specs=(
            P("tm", None, "row", None),
            P("tm", None, "row", None),
            P("tm", None, "row", None),
            P("tm", None, None, None),
            P("tm", None),
            P("row", None),
            P(),
            P(),
            P("row"),
        ),
        out_specs=(P("tm", None, "row", None), P("tm", None, "row", None)),
        check_vma=False,
    )
```
